32 devices in a mesh: group: 4 (over y, x), depth: 2 (over core), mp: 4 (over z).
Axes of the slice: x: 2, y: 2, z: 4, core: 2. Of those that a mesh axis runs over, the one named last changes fastest.
Arguments:
- states: bfloat16 [64, 4096], P(('group', 'depth', 'mp')), may hold values from -6 to 6
- queries: bfloat16 [64, 32, 128], P('group', 'mp'), may hold values from -6 to 6
- new_keys: bfloat16 [64, 8, 128], P('group', 'mp'), may hold values from -18 to 18
- new_values: bfloat16 [64, 8, 128], P('group', 'mp'), may hold values from -24 to 24
- text_keys: bfloat16 [64, 8, 512, 128], P('group', 'mp', 'depth'), may hold values from -6 to 6
- text_values: bfloat16 [64, 8, 512, 128], P('group', 'mp', 'depth'), may hold values from -24 to 24
- text_length: int32 [64], P('group'), may hold values from 2 to 512
- image_keys: bfloat16 [32, 8, 576, 128], P('group', 'mp'), may hold values from -6 to 6
- image_values: bfloat16 [32, 8, 576, 128], P('group', 'mp'), may hold values from -24 to 24
- image_slot: int32 [32], replicated, may hold values from 0 to 31, as said below
- block_list: int32 [4, 32], replicated, may hold values from 0 to 31, as said below
- block_count: int32 [4], replicated, may hold values from 16 to 32, as said below
- image_first: int32 [64], P('group'), may hold values from 0 to 31, as said below
- image_count: int32 [64], P('group'), may hold values from 1 to 2
- out_weight: bfloat16 [4096, 4096], P('mp'), may hold values from -0.09375 to 0.09375
- norm_gain: float32 [4096], replicated, may hold values from 0.5 to 1.5
- gate_weight: bfloat16 [4096, 14336], P(None, ('group', 'mp')), may hold values from -0.09375 to 0.09375
- up_weight: bfloat16 [4096, 14336], P(None, ('group', 'mp')), may hold values from -0.09375 to 0.09375
- down_weight: bfloat16 [14336, 4096], P(('group', 'mp')), may hold values from -0.046875 to 0.046875
Outputs:
- attention: bfloat16 [64, 32, 128], P(('group', 'depth'), 'mp')
- layer_out: bfloat16 [64, 4096], P(('group', 'depth', 'mp'))
The draws below stay inside these ranges and needn't reach their ends.
Inputs may be any that keep to these rules, and one draw needn't show every extreme that they name: `image_slot`: a permutation. The owner group of hash k is image_slot[k] // 8. `block_list`: the hashes of one group's list are distinct. Among one group's places with the same remainder modulo 2, at most 4 belongs to any one owner group; some group has block_count 32, and there every owner group holds exactly 4 place of every remainder. `block_count`: the sum of image_count over the group's requests. The requests of a group take consecutive list places in request order: image_first is the sum of image_count over the group's earlier requests.
All inputs are finite; a program needn't handle non-finite values.
Results may differ from the reference program's by a relative error of at most 0.012.
Values may be sent and summed in bfloat16 or wider, within the bound.
A program may use at most 128 MiB of HBM per device.

```python
import math
import jax
import jax.numpy as jnp
from jax import lax

D = 4096
HQ = 32
KVH = 8
HD = 128
FF = 14336
PATCHES = 576
REQ = 16
IMG_DEV = 8
GROUPS = 4
DEPTHS = 2
BATCH = 64
LTEXT = 512
IMAGES = 32
LIST = 32
CAP = 4


def routing_plan(key):
    slot_order = jax.random.permutation(jax.random.fold_in(key, 101), IMAGES).astype(jnp.int32)
    hash_at = jnp.argsort(slot_order, stable=True).astype(jnp.int32)
    picked = jax.random.randint(jax.random.fold_in(key, 102), (GROUPS, REQ), 1, 3, dtype=jnp.int32)
    fullest = jax.random.randint(jax.random.fold_in(key, 103), (), 0, GROUPS, dtype=jnp.int32)
    picked = jnp.where(jnp.arange(GROUPS, dtype=jnp.int32)[:, None] == fullest, 2, picked).astype(jnp.int32)
    starts = (jnp.cumsum(picked, axis=1) - picked).astype(jnp.int32)
    totals = jnp.sum(picked, axis=1).astype(jnp.int32)
    order_keys = jax.random.split(jax.random.fold_in(key, 104), GROUPS * DEPTHS)
    orderings = jax.vmap(lambda single: jax.random.permutation(single, GROUPS * CAP))(order_keys)
    orderings = orderings.reshape(GROUPS, DEPTHS, GROUPS * CAP).astype(jnp.int32)
    owners = orderings % GROUPS
    copy_index = orderings // GROUPS
    pick_keys = jax.random.split(jax.random.fold_in(key, 105), GROUPS * GROUPS)
    inner_orders = jax.vmap(lambda single: jax.random.permutation(single, IMG_DEV))(pick_keys)
    inner_orders = inner_orders.reshape(GROUPS, GROUPS, IMG_DEV).astype(jnp.int32)
    column = jnp.arange(DEPTHS, dtype=jnp.int32)[None, :, None] * CAP + copy_index
    group_axis = jnp.arange(GROUPS, dtype=jnp.int32)[:, None, None]
    within = inner_orders[group_axis, owners, column]
    slot_rows = owners * IMG_DEV + within
    hashes = hash_at[slot_rows]
    listing = jnp.transpose(hashes, (0, 2, 1)).reshape(GROUPS, LIST).astype(jnp.int32)
    return (slot_order, listing, totals, starts.reshape(-1), picked.reshape(-1))


def draw_image_slot(key, part):
    return routing_plan(key)[0]


def draw_block_list(key, part):
    return routing_plan(key)[1]


def draw_block_count(key, part):
    return routing_plan(key)[2]


def draw_image_first(key, part):
    return routing_plan(key)[3]


def draw_image_count(key, part):
    return routing_plan(key)[4]


def draw_queries(key, part):
    values = jnp.clip(jax.random.normal(jax.random.fold_in(key, 203), (BATCH, HQ, HD), jnp.float32), -6.0, 6.0)
    return values.astype(jnp.bfloat16)


def draw_text_keys(key, part):
    values = jnp.clip(jax.random.normal(jax.random.fold_in(key, 205), (BATCH, KVH, LTEXT, HD), jnp.float32), -6.0, 6.0)
    return values.astype(jnp.bfloat16)


def with_ends(drawn, rng, low, largest):
    longest = drawn.shape.index(max(drawn.shape))
    spots = []
    for shift in (0, 1):
        where = [jax.random.randint(jax.random.fold_in(rng, axis), (), 0, length) for axis, length in enumerate(drawn.shape)]
        where[longest] = (where[longest] + shift) % drawn.shape[longest]
        spots.append(tuple(where))
    return drawn.at[spots[0]].set(low).at[spots[1]].set(largest)


def steps_of(stream_key, shape, shards, least, high):
    level, own = 1.0, jax.random.fold_in(stream_key, 6)
    for position, parts in shards:
        draws = jnp.exp(jax.random.uniform(jax.random.fold_in(own, position), (parts,), jnp.float32, least / len(shards), high / len(shards)))
        level = level * jnp.repeat(draws, shape[position] // parts).reshape([-1 if axis == position else 1 for axis in range(len(shape))])
    return level


def gaussian(rng, extent, scale, limit, cuts=(), kind=jnp.bfloat16):
    factor_of = steps_of(rng, extent, cuts, -0.22, 0.18) if cuts else 1.0
    array = jax.random.normal(rng, extent, jnp.float32) * scale * factor_of
    return jnp.minimum(jnp.maximum(array, -limit), limit).astype(kind)


def setup_inputs(seed: int = 0) -> dict:
    keys = jax.random.split(jax.random.key(seed), 20)
    states = gaussian(keys[0], (BATCH, D), 1.0, 6.0, ((0, 32),))
    queries = draw_queries(jax.random.fold_in(keys[19], 71), 0)
    new_keys = gaussian(keys[2], (BATCH, KVH, HD), 3.0, 18.0, ((0, 4), (1, 4)))
    new_values = gaussian(keys[3], (BATCH, KVH, HD), 4.0, 24.0, ((0, 4), (1, 4)))
    text_keys = draw_text_keys(jax.random.fold_in(keys[19], 71), 0)
    text_values = gaussian(keys[5], (BATCH, KVH, LTEXT, HD), 4.0, 24.0, ((0, 4), (1, 4), (2, 2)))
    text_length = with_ends(jax.random.randint(keys[6], (BATCH,), 2, LTEXT + 1), jax.random.fold_in(keys[6], 1), 2, LTEXT).astype(jnp.int32)
    image_keys = gaussian(keys[7], (IMAGES, KVH, PATCHES, HD), 1.0, 6.0, ((0, 4), (1, 4)))
    image_values = gaussian(keys[8], (IMAGES, KVH, PATCHES, HD), 4.0, 24.0, ((0, 4), (1, 4)))
    image_slot = draw_image_slot(jax.random.fold_in(keys[19], 71), 0)
    block_list = draw_block_list(jax.random.fold_in(keys[19], 71), 0)
    block_count = draw_block_count(jax.random.fold_in(keys[19], 71), 0)
    image_first = draw_image_first(jax.random.fold_in(keys[19], 71), 0)
    image_count = draw_image_count(jax.random.fold_in(keys[19], 71), 0)
    out_weight = gaussian(keys[14], (HQ * HD, D), (HQ * HD) ** -0.5, 0.09375, ((0, 4),))
    norm_gain = jnp.clip(1.0 + 0.1 * jax.random.normal(keys[15], (D,), jnp.float32), 0.5, 1.5)
    gate_weight = gaussian(keys[16], (D, FF), D ** -0.5, 0.09375, ((1, 16),))
    up_weight = gaussian(keys[17], (D, FF), D ** -0.5, 0.09375, ((1, 16),))
    down_weight = gaussian(keys[18], (FF, D), FF ** -0.5, 0.046875, ((0, 16),))
    return dict(states=states, queries=queries, new_keys=new_keys, new_values=new_values, text_keys=text_keys, text_values=text_values, text_length=text_length, image_keys=image_keys, image_values=image_values, image_slot=image_slot, block_list=block_list, block_count=block_count, image_first=image_first, image_count=image_count, out_weight=out_weight, norm_gain=norm_gain, gate_weight=gate_weight, up_weight=up_weight, down_weight=down_weight)


LOG_TWO = math.log(2.0)
MASKED_SCORE = -1e+30
NORM_EPSILON = 1e-05

def reference(states, queries, new_keys, new_values, text_keys, text_values, text_length, image_keys, image_values, image_slot, block_list, block_count, image_first, image_count, out_weight, norm_gain, gate_weight, up_weight, down_weight):
    share = HQ // KVH
    scaling = 1.0 / math.sqrt(HD)

    def one_group(group_index):
        offset = (group_index * REQ).astype(jnp.int32)
        grouped = lax.dynamic_slice_in_dim(queries, offset, REQ, 0).astype(jnp.float32).reshape(REQ, KVH, share, HD)
        text_key_rows = lax.dynamic_slice_in_dim(text_keys, offset, REQ, 0).astype(jnp.float32)
        text_value_rows = lax.dynamic_slice_in_dim(text_values, offset, REQ, 0).astype(jnp.float32)
        new_key_rows = lax.dynamic_slice_in_dim(new_keys, offset, REQ, 0).astype(jnp.float32)
        new_value_rows = lax.dynamic_slice_in_dim(new_values, offset, REQ, 0).astype(jnp.float32)
        lengths = lax.dynamic_slice_in_dim(text_length, offset, REQ, 0)
        starts = lax.dynamic_slice_in_dim(image_first, offset, REQ, 0)
        image_total = lax.dynamic_slice_in_dim(image_count, offset, REQ, 0)
        hashes = block_list[group_index]
        slot_rows = jnp.take(image_slot, hashes, axis=0)
        image_key_rows = jnp.take(image_keys, slot_rows, axis=0).astype(jnp.float32)
        image_value_rows = jnp.take(image_values, slot_rows, axis=0).astype(jnp.float32)
        text_scores = jnp.einsum('rhgd,rhpd->rhgp', grouped, text_key_rows) * scaling
        new_scores = jnp.einsum('rhgd,rhd->rhg', grouped, new_key_rows) * scaling
        image_scores = jnp.einsum('rhgd,jhpd->rhgjp', grouped, image_key_rows) * scaling
        image_scores = image_scores.reshape(REQ, KVH, share, LIST * PATCHES)
        scores = jnp.concatenate([text_scores, new_scores[..., None], image_scores], axis=-1)
        text_mask = jnp.arange(LTEXT, dtype=jnp.int32)[None, :] < lengths[:, None]
        positions = jnp.arange(LIST, dtype=jnp.int32)[None, :]
        image_mask = (positions >= starts[:, None]) & (positions < (starts + image_total)[:, None]) & (positions < block_count[group_index])
        image_mask = jnp.repeat(image_mask, PATCHES, axis=1)
        new_mask = jnp.ones((REQ, 1), dtype=bool)
        allowed = jnp.concatenate([text_mask, new_mask, image_mask], axis=1)[:, None, None, :]
        masked = jnp.where(allowed, scores, MASKED_SCORE)
        highest = lax.optimization_barrier(jnp.max(masked, axis=-1, keepdims=True))
        levels = jnp.floor(highest / LOG_TWO)
        weights = jnp.where(allowed, jnp.exp(scores - LOG_TWO * levels), 0.0).astype(jnp.bfloat16)
        weights = lax.optimization_barrier(weights).astype(jnp.float32)
        totals = lax.optimization_barrier(jnp.sum(weights, axis=-1))
        text_weights = weights[..., :LTEXT]
        new_weights = weights[..., LTEXT]
        image_weights = weights[..., LTEXT + 1:].reshape(REQ, KVH, share, LIST, PATCHES)
        summed = jnp.einsum('rhgp,rhpd->rhgd', text_weights, text_value_rows)
        summed = summed + new_weights[..., None] * new_value_rows[:, :, None, :]
        summed = summed + jnp.einsum('rhgjp,jhpd->rhgd', image_weights, image_value_rows)
        return (summed / totals[..., None]).reshape(REQ, HQ, HD).astype(jnp.bfloat16)
    attention = lax.map(one_group, jnp.arange(GROUPS, dtype=jnp.int32)).reshape(BATCH, HQ, HD)
    projected = jnp.dot(attention.reshape(BATCH, HQ * HD), out_weight, preferred_element_type=jnp.float32)
    residual = states.astype(jnp.float32) + projected
    spread = lax.optimization_barrier(jnp.mean(residual * residual, axis=-1, keepdims=True))
    normed = (residual * lax.rsqrt(spread + NORM_EPSILON) * norm_gain.astype(jnp.float32)).astype(jnp.bfloat16)
    gate_term = jnp.dot(normed, gate_weight, preferred_element_type=jnp.float32)
    up_term = jnp.dot(normed, up_weight, preferred_element_type=jnp.float32)
    hidden = (jax.nn.silu(gate_term) * up_term).astype(jnp.bfloat16)
    result = residual + jnp.dot(hidden, down_weight, preferred_element_type=jnp.float32)
    return (attention, result.astype(jnp.bfloat16))
```

```python
import functools
import math

import jax
import jax.numpy as jnp
from jax import lax
from jax.experimental import pallas as pl
from jax.experimental.pallas import tpu as pltpu
from jax.sharding import PartitionSpec as P

LOG_TWO = math.log(2.0)
MASKED_SCORE = -1e30
NORM_EPSILON = 1e-05
READS = 2
MESH = pl.DeviceIdType.MESH
F32 = jnp.float32
BF16 = jnp.bfloat16
NT = (((1,), (1,)), ((), ()))


def tile_of(size, most):
    for tile in (most, most // 2, most // 4):
        if size % tile == 0:
            return tile
    return size


def kernel(
    dims,
    states,
    queries,
    new_keys,
    new_values,
    norm_gain,
    text_length,
    image_slot,
    block_list,
    block_count,
    image_first,
    image_count,
    text_keys_hbm,
    text_values_hbm,
    image_keys_hbm,
    image_values_hbm,
    out_weight_hbm,
    gate_hbm,
    up_hbm,
    down_hbm,
    attention_out,
    layer_out,
    text_keys,
    text_values,
    image_keys,
    image_values,
    out_weight,
    gate,
    up,
    down,
    chosen,
    codes,
    readers,
    query_send,
    query_recv,
    text_scores,
    new_scores,
    text_weights,
    text_part,
    text_recv,
    image_scores,
    image_weights,
    image_send,
    image_recv,
    merged,
    flat,
    projected,
    proj_send,
    proj_recv,
    residual,
    norm_all,
    tokens,
    tokens_low,
    gate_sum,
    up_sum,
    hidden,
    down_sum,
    down_send,
    down_recv,
    load_sem,
    query_ssem,
    query_rsem,
    text_ssem,
    text_rsem,
    image_ssem,
    image_rsem,
    proj_ssem,
    proj_rsem,
    norm_ssem,
    norm_rsem,
    down_ssem,
    down_rsem,
):
    groups, depths, mps = dims
    pieces = groups * mps
    g = lax.axis_index("group")
    d = lax.axis_index("depth")
    m = lax.axis_index("mp")
    me = g * mps + m
    requests, heads, width = queries.shape
    kv_heads, span = text_keys.shape[1], text_keys.shape[2]
    share = heads // kv_heads
    stored, patches = image_keys.shape[0], image_keys.shape[2]
    listed = block_list.shape[1]
    steps = listed // depths
    copies = listed // (depths * groups)
    per_depth = requests // depths
    rows = states.shape[0]
    model = states.shape[1]
    scaling = 1.0 / math.sqrt(width)

    pairs = (
        (text_keys_hbm, text_keys),
        (text_values_hbm, text_values),
        (image_keys_hbm, image_keys),
        (image_values_hbm, image_values),
        (out_weight_hbm, out_weight),
        (gate_hbm, gate),
        (up_hbm, up),
        (down_hbm, down),
    )
    loads = [pltpu.make_async_copy(a, b, load_sem.at[i]) for i, (a, b) in enumerate(pairs)]
    for load in loads[:5]:
        load.start()

    barrier = pltpu.get_barrier_semaphore()

    def greet_piece(k, carry):
        peer = lax.rem(me + k, pieces)
        pl.semaphore_signal(
            barrier, inc=1, device_id=(peer // mps, d, lax.rem(peer, mps)), device_id_type=MESH
        )
        return carry

    lax.fori_loop(1, pieces, greet_piece, 0)
    for e in range(1, depths):

        def greet_depth(k, carry):
            pl.semaphore_signal(
                barrier,
                inc=1,
                device_id=(lax.rem(g + k, groups), lax.rem(d + e, depths), m),
                device_id_type=MESH,
            )
            return carry

        lax.fori_loop(0, groups, greet_depth, 0)

    own_count = block_count[g]

    def place_step(i, counts):
        out = []
        for p in range(depths):
            place = i * depths + p
            owner = image_slot[block_list[g, place]] // stored
            rank = jnp.int32(0)
            for o in range(groups):
                rank = jnp.where(owner == o, counts[p * groups + o], rank)
            codes[place] = jnp.minimum(owner * copies + rank, groups * copies - 1)
            live = (place < own_count).astype(jnp.int32)
            for o in range(groups):
                out.append(counts[p * groups + o] + jnp.where(owner == o, live, 0))
        return tuple(out)

    lax.fori_loop(0, steps, place_step, (jnp.int32(0),) * (depths * groups))

    def reader_step(r, found):
        for k in range(READS):
            place = image_first[r] + k
            held = jnp.minimum(place, listed - 1)
            good = (k < image_count[r]) & (place < own_count) & (lax.rem(place, depths) == d)
            code = jnp.where(good, codes[held], -1)
            found = tuple(jnp.where(code == i, r, old) for i, old in enumerate(found))
        return found

    found = lax.fori_loop(0, requests, reader_step, (jnp.int32(0),) * (groups * copies))
    for i, reader in enumerate(found):
        readers[i] = reader
    for o in range(groups):
        for c in range(copies):
            query_send[o, c] = queries[readers[o * copies + c]]
    query_recv[g] = query_send[g]

    pl.semaphore_wait(barrier, pieces - 1 + (depths - 1) * groups)

    def query_copy(peer, slot):
        return pltpu.make_async_remote_copy(
            src_ref=query_send.at[peer],
            dst_ref=query_recv.at[slot],
            send_sem=query_ssem.at[peer],
            recv_sem=query_rsem.at[slot],
            device_id=(peer, d, m),
            device_id_type=MESH,
        )

    def over(count, action):
        def body(k, carry):
            action(k)
            return carry

        lax.fori_loop(1, count, body, 0)

    over(groups, lambda k: query_copy(lax.rem(g + k, groups), g).start())

    def serve_step(i, state):
        place = i * depths + d
        out = []
        for s in range(groups):
            rank, picked = state[s]
            slot = image_slot[block_list[s, place]]
            hit = ((slot // stored) == g) & (place < block_count[s])
            within = lax.rem(slot, stored)
            target = jnp.where(hit, rank, -1)
            picked = tuple(jnp.where(target == c, within, old) for c, old in enumerate(picked))
            out.append((rank + hit.astype(jnp.int32), picked))
        return tuple(out)

    zero = jnp.int32(0)
    served = lax.fori_loop(0, steps, serve_step, ((zero, (zero,) * copies),) * groups)
    for s in range(groups):
        for c in range(copies):
            chosen[s * copies + c] = served[s][1][c]

    def by_head(parts):
        result = parts[0]
        row = lax.broadcasted_iota(jnp.int32, result.shape, 0)
        for h in range(1, kv_heads):
            result = jnp.where(row >= h * share, parts[h], result)
        return result

    def spread_rows(small):
        return by_head(
            [jnp.broadcast_to(small[h : h + 1, :], (heads, width)) for h in range(kv_heads)]
        )

    loads[0].wait()
    lanes = lax.broadcasted_iota(jnp.int32, (heads, span), 1) + d * span

    def text_first(r, carry):
        q = queries[r]
        score = by_head(
            [
                lax.dot_general(q, text_keys[r, h], NT, preferred_element_type=F32)
                for h in range(kv_heads)
            ]
        )
        text_scores[r] = jnp.where(lanes < text_length[r], score * scaling, MASKED_SCORE)
        key = spread_rows(new_keys[r].astype(F32))
        new_score = jnp.sum(q.astype(F32) * key, axis=-1, keepdims=True) * scaling
        new_scores[r] = jnp.broadcast_to(new_score, (heads, width))
        return carry

    lax.fori_loop(0, requests, text_first, 0, unroll=4)
    is_first = jnp.full((requests, heads, width), d, jnp.int32) == 0
    score = text_scores[...]
    fresh = jnp.where(is_first, new_scores[...], MASKED_SCORE)
    top = jnp.maximum(jnp.max(score, axis=-1, keepdims=True), fresh)
    level = jnp.floor(top / LOG_TWO)
    text_part[:, 1] = level
    weight = jnp.where(
        score > 0.5 * MASKED_SCORE, jnp.exp(score - LOG_TWO * level[:, :, :1]), 0.0
    ).astype(BF16)
    text_weights[...] = weight
    fresh_weight = jnp.where(is_first, jnp.exp(new_scores[...] - LOG_TWO * level), 0.0)
    fresh_weight = fresh_weight.astype(BF16).astype(F32)
    new_scores[...] = fresh_weight
    text_part[:, 2] = jnp.sum(weight.astype(F32), axis=-1, keepdims=True) + fresh_weight
    loads[1].wait()

    def text_second(r, carry):
        w = text_weights[r]
        value = by_head(
            [
                jnp.dot(w, text_values[r, h], preferred_element_type=F32)
                for h in range(kv_heads)
            ]
        )
        text_part[r, 0] = value + new_scores[r] * spread_rows(new_values[r].astype(F32))
        return carry

    lax.fori_loop(0, requests, text_second, 0, unroll=4)

    def text_copy(peer, slot):
        return pltpu.make_async_remote_copy(
            src_ref=text_part.at[pl.ds(peer * per_depth, per_depth)],
            dst_ref=text_recv.at[slot],
            send_sem=text_ssem.at[peer],
            recv_sem=text_rsem.at[slot],
            device_id=(g, peer, m),
            device_id_type=MESH,
        )

    over(depths, lambda k: text_copy(lax.rem(d + k, depths), d).start())
    for load in loads[5:]:
        load.start()

    loads[2].wait()
    loads[3].wait()

    def serve(s):
        slots = [chosen[s * copies + c] for c in range(copies)]
        for c in range(copies):
            q = query_recv[s, c]
            image_scores[c] = scaling * by_head(
                [
                    lax.dot_general(q, image_keys[slots[c], h], NT, preferred_element_type=F32)
                    for h in range(kv_heads)
                ]
            )
        score = image_scores[...]
        level = jnp.floor(jnp.max(score, axis=-1, keepdims=True) / LOG_TWO)
        weight = jnp.exp(score - LOG_TWO * level).astype(BF16)
        image_weights[...] = weight
        total = jnp.sum(weight.astype(F32), axis=-1, keepdims=True)
        image_send[s, :, 1] = jnp.broadcast_to(level, (copies, heads, width))
        image_send[s, :, 2] = jnp.broadcast_to(total, (copies, heads, width))
        for c in range(copies):
            w = image_weights[c]
            image_send[s, c, 0] = by_head(
                [
                    jnp.dot(w, image_values[slots[c], h], preferred_element_type=F32)
                    for h in range(kv_heads)
                ]
            )

    def image_copy(peer, depth, slot, slot_depth):
        return pltpu.make_async_remote_copy(
            src_ref=image_send.at[peer],
            dst_ref=image_recv.at[slot_depth, pl.ds(slot * copies, copies)],
            send_sem=image_ssem.at[depth, peer],
            recv_sem=image_rsem.at[slot_depth, slot],
            device_id=(peer, depth, m),
            device_id_type=MESH,
        )

    serve(g)
    image_recv[d, pl.ds(g * copies, copies)] = image_send[g]
    for e in range(1, depths):
        image_copy(g, lax.rem(d + e, depths), g, d).start()

    def serve_other(k):
        s = lax.rem(g + k, groups)
        query_copy(s, s).wait_recv()
        serve(s)
        for e in range(depths):
            image_copy(s, lax.rem(d + e, depths), g, d).start()

    over(groups, serve_other)

    over(depths, lambda k: text_copy(lax.rem(d + k, depths), lax.rem(d + k, depths)).wait_recv())
    for e in range(1, depths):
        other = lax.rem(d + e, depths)
        image_copy(g, other, g, other).wait_recv()

    def image_arrival(k):
        s = lax.rem(g + k, groups)
        for e in range(depths):
            other = lax.rem(d + e, depths)
            image_copy(s, other, s, other).wait_recv()

    over(groups, image_arrival)
    text_recv[d] = text_part[pl.ds(d * per_depth, per_depth)]

    def merge(i, carry):
        r = d * per_depth + i
        parts = [tuple(text_recv[e, i, n] for n in range(3)) for e in range(depths)]
        for k in range(READS):
            place = image_first[r] + k
            good = (k < image_count[r]) & (place < own_count)
            held = jnp.minimum(place, listed - 1)
            code = codes[held]
            at = lax.rem(held, depths)
            live = jnp.full((heads, width), good.astype(jnp.int32), jnp.int32) == 1
            parts.append(
                (
                    jnp.where(live, image_recv[at, code, 0], 0.0),
                    jnp.where(live, image_recv[at, code, 1], MASKED_SCORE),
                    jnp.where(live, image_recv[at, code, 2], 0.0),
                )
            )
        highest = functools.reduce(jnp.maximum, [part[1] for part in parts])
        factors = [jnp.exp2(part[1] - highest) for part in parts]
        total = sum(part[2] * factor for part, factor in zip(parts, factors))
        value = sum(part[0] * factor for part, factor in zip(parts, factors)) / total
        merged[i] = value
        attention_out[i] = value.astype(BF16)
        return carry

    lax.fori_loop(0, per_depth, merge, 0, unroll=2)
    for h in range(heads):
        flat[:, h * width : (h + 1) * width] = merged[:, h, :]

    loads[4].wait()
    low = flat[...].astype(BF16)
    tile = tile_of(model, 512)

    def project(n, carry):
        columns = pl.ds(pl.multiple_of(n * tile, tile), tile)
        projected[:, columns] = jnp.dot(low, out_weight[:, columns], preferred_element_type=F32)
        return carry

    lax.fori_loop(0, model // tile, project, 0)
    for i in range(mps):
        proj_send[i] = projected[i * rows : (i + 1) * rows, :].astype(proj_send.dtype)

    def proj_copy(peer, slot):
        return pltpu.make_async_remote_copy(
            src_ref=proj_send.at[peer],
            dst_ref=proj_recv.at[slot],
            send_sem=proj_ssem.at[peer],
            recv_sem=proj_rsem.at[slot],
            device_id=(g, d, peer),
            device_id_type=MESH,
        )

    over(mps, lambda k: proj_copy(lax.rem(m + k, mps), m).start())
    proj_recv[m] = proj_send[m]
    over(mps, lambda k: proj_copy(lax.rem(m + k, mps), lax.rem(m + k, mps)).wait_recv())
    total = states[...].astype(F32)
    for i in range(mps):
        total = total + proj_recv[i].astype(F32)
    residual[...] = total
    spread = jnp.mean(total * total, axis=-1, keepdims=True)
    norm_all[me] = (total * lax.rsqrt(spread + NORM_EPSILON) * norm_gain[...]).astype(BF16)

    def norm_copy(peer, slot):
        return pltpu.make_async_remote_copy(
            src_ref=norm_all.at[me],
            dst_ref=norm_all.at[slot],
            send_sem=norm_ssem.at[peer],
            recv_sem=norm_rsem.at[slot],
            device_id=(peer // mps, d, lax.rem(peer, mps)),
            device_id_type=MESH,
        )

    over(pieces, lambda k: norm_copy(lax.rem(me + k, pieces), me).start())
    loads[5].wait()
    loads[6].wait()
    loads[7].wait()
    over(pieces, lambda k: norm_copy(lax.rem(me + k, pieces), lax.rem(me + k, pieces)).wait_recv())
    for i in range(pieces):
        tokens[i * rows : (i + 1) * rows, :] = norm_all[i].astype(F32)
    tokens_low[...] = tokens[...].astype(BF16)
    gate_sum[...] = jnp.zeros_like(gate_sum)
    up_sum[...] = jnp.zeros_like(up_sum)

    def expand(k, carry):
        part = pl.ds(pl.multiple_of(k * tile, tile), tile)
        x = tokens_low[:, part]
        gate_sum[...] += jnp.dot(x, gate[part, :], preferred_element_type=F32)
        up_sum[...] += jnp.dot(x, up[part, :], preferred_element_type=F32)
        return carry

    lax.fori_loop(0, model // tile, expand, 0)
    v = gate_sum[...]
    hidden[...] = (v / (1.0 + jnp.exp(-v)) * up_sum[...]).astype(BF16)

    def contract(n, carry):
        columns = pl.ds(pl.multiple_of(n * tile, tile), tile)
        down_sum[:, columns] = jnp.dot(hidden[...], down[:, columns], preferred_element_type=F32)
        return carry

    lax.fori_loop(0, model // tile, contract, 0)
    for i in range(pieces):
        down_send[i] = down_sum[i * rows : (i + 1) * rows, :].astype(down_send.dtype)

    def down_copy(peer, slot):
        return pltpu.make_async_remote_copy(
            src_ref=down_send.at[peer],
            dst_ref=down_recv.at[slot],
            send_sem=down_ssem.at[peer],
            recv_sem=down_rsem.at[slot],
            device_id=(peer // mps, d, lax.rem(peer, mps)),
            device_id_type=MESH,
        )

    over(pieces, lambda k: down_copy(lax.rem(me + k, pieces), me).start())
    down_recv[me] = down_send[me]
    over(pieces, lambda k: down_copy(lax.rem(me + k, pieces), lax.rem(me + k, pieces)).wait_recv())

    def add_piece(i, total):
        return total + down_recv[i].astype(F32)

    layer_out[...] = lax.fori_loop(0, pieces, add_piece, residual[...]).astype(BF16)

    over(groups, lambda k: query_copy(lax.rem(g + k, groups), g).wait_send())
    over(depths, lambda k: text_copy(lax.rem(d + k, depths), d).wait_send())
    for e in range(1, depths):
        image_copy(g, lax.rem(d + e, depths), g, d).wait_send()

    def image_gone(k):
        for e in range(depths):
            image_copy(lax.rem(g + k, groups), lax.rem(d + e, depths), g, d).wait_send()

    over(groups, image_gone)
    over(mps, lambda k: proj_copy(lax.rem(m + k, mps), m).wait_send())
    over(pieces, lambda k: norm_copy(lax.rem(me + k, pieces), me).wait_send())
    over(pieces, lambda k: down_copy(lax.rem(me + k, pieces), me).wait_send())


def on_device(
    states,
    queries,
    new_keys,
    new_values,
    text_keys,
    text_values,
    text_length,
    image_keys,
    image_values,
    image_slot,
    block_list,
    block_count,
    image_first,
    image_count,
    out_weight,
    norm_gain,
    gate_weight,
    up_weight,
    down_weight,
):
    groups = lax.axis_size("group")
    depths = lax.axis_size("depth")
    mps = lax.axis_size("mp")
    pieces = groups * mps
    requests, heads, width = queries.shape
    listed = block_list.shape[1]
    copies = listed // (depths * groups)
    per_depth = requests // depths
    rows, model = states.shape
    units = gate_weight.shape[1]
    span = text_keys.shape[2]
    patches = image_keys.shape[2]
    dma = pltpu.SemaphoreType.DMA
    vmem = pl.BlockSpec(memory_space=pltpu.VMEM)
    smem = pl.BlockSpec(memory_space=pltpu.SMEM)
    hbm = pl.BlockSpec(memory_space=pl.ANY)
    big = (
        text_keys,
        text_values,
        image_keys,
        image_values,
        out_weight,
        gate_weight,
        up_weight,
        down_weight,
    )
    scratch = [pltpu.VMEM(a.shape, a.dtype) for a in big]
    scratch += [
        pltpu.SMEM((groups * copies,), jnp.int32),
        pltpu.SMEM((listed,), jnp.int32),
        pltpu.SMEM((groups * copies,), jnp.int32),
        pltpu.VMEM((groups, copies, heads, width), BF16),
        pltpu.VMEM((groups, copies, heads, width), BF16),
        pltpu.VMEM((requests, heads, span), F32),
        pltpu.VMEM((requests, heads, width), F32),
        pltpu.VMEM((requests, heads, span), BF16),
        pltpu.VMEM((requests, 3, heads, width), F32),
        pltpu.VMEM((depths, per_depth, 3, heads, width), F32),
        pltpu.VMEM((copies, heads, patches), F32),
        pltpu.VMEM((copies, heads, patches), BF16),
        pltpu.VMEM((groups, copies, 3, heads, width), F32),
        pltpu.VMEM((depths, groups * copies, 3, heads, width), F32),
        pltpu.VMEM((per_depth, heads, width), F32),
        pltpu.VMEM((per_depth, heads * width), F32),
        pltpu.VMEM((per_depth, model), F32),
        pltpu.VMEM((mps, rows, model), F32),
        pltpu.VMEM((mps, rows, model), F32),
        pltpu.VMEM((rows, model), F32),
        pltpu.VMEM((pieces, rows, model), BF16),
        pltpu.VMEM((pieces * rows, model), F32),
        pltpu.VMEM((pieces * rows, model), BF16),
        pltpu.VMEM((pieces * rows, units), F32),
        pltpu.VMEM((pieces * rows, units), F32),
        pltpu.VMEM((pieces * rows, units), BF16),
        pltpu.VMEM((pieces * rows, model), F32),
        pltpu.VMEM((pieces, rows, model), BF16),
        pltpu.VMEM((pieces, rows, model), BF16),
        dma((len(big),)),
        dma((groups,)),
        dma((groups,)),
        dma((depths,)),
        dma((depths,)),
        dma((depths, groups)),
        dma((depths, groups)),
        dma((mps,)),
        dma((mps,)),
        dma((pieces,)),
        dma((pieces,)),
        dma((pieces,)),
        dma((pieces,)),
    ]
    return pl.pallas_call(
        functools.partial(kernel, (groups, depths, mps)),
        out_shape=(
            jax.ShapeDtypeStruct((per_depth, heads, width), BF16),
            jax.ShapeDtypeStruct((rows, model), BF16),
        ),
        in_specs=[vmem] * 5 + [smem] * 6 + [hbm] * 8,
        out_specs=(vmem, vmem),
        scratch_shapes=scratch,
        compiler_params=pltpu.CompilerParams(
            collective_id=0, has_side_effects=True, vmem_limit_bytes=67043328
        ),
    )(
        states,
        queries,
        new_keys,
        new_values,
        norm_gain.reshape(1, model),
        text_length,
        image_slot,
        block_list,
        block_count,
        image_first,
        image_count,
        *big,
    )


def solution(mesh):
    placed = (
        P(("group", "depth", "mp"), None),
        P("group", "mp", None),
        P("group", "mp", None),
        P("group", "mp", None),
        P("group", "mp", "depth", None),
        P("group", "mp", "depth", None),
        P("group"),
        P("group", "mp", None, None),
        P("group", "mp", None, None),
        P(),
        P(),
        P(),
        P("group"),
        P("group"),
        P("mp", None),
        P(),
        P(None, ("group", "mp")),
        P(None, ("group", "mp")),
        P(("group", "mp"), None),
    )
    return jax.shard_map(
        on_device,
        mesh=mesh,
        in_specs=placed,
        out_specs=(P(("group", "depth"), "mp", None), P(("group", "depth", "mp"), None)),
        check_vma=False,
    )
```

```python
import functools
import math

import jax
import jax.numpy as jnp
from jax import lax
from jax.experimental import pallas as pl
from jax.experimental.pallas import tpu as pltpu
from jax.sharding import PartitionSpec as P

LOG_TWO = math.log(2.0)
MASKED_SCORE = -1e30
NORM_EPSILON = 1e-05
READS = 2
MESH = pl.DeviceIdType.MESH
F32 = jnp.float32
BF16 = jnp.bfloat16
NT = (((1,), (1,)), ((), ()))


def tile_of(size, most):
    for tile in (most, most // 2, most // 4):
        if size % tile == 0:
            return tile
    return size


def kernel(
    dims,
    states,
    queries,
    new_keys,
    new_values,
    norm_gain,
    text_length,
    image_slot,
    block_list,
    block_count,
    image_first,
    image_count,
    text_keys_hbm,
    text_values_hbm,
    image_keys_hbm,
    image_values_hbm,
    out_weight_hbm,
    gate_hbm,
    up_hbm,
    down_hbm,
    attention_out,
    layer_out,
    text_keys,
    text_values,
    image_keys,
    image_values,
    out_weight,
    gate,
    up,
    down,
    chosen,
    codes,
    readers,
    query_send,
    query_recv,
    text_scores,
    new_scores,
    text_weights,
    text_part,
    text_recv,
    image_scores,
    image_weights,
    image_send,
    stat_send,
    image_recv,
    stat_recv,
    merged,
    flat,
    projected,
    proj_send,
    proj_recv,
    residual,
    norm_all,
    tokens,
    tokens_low,
    gate_sum,
    up_sum,
    hidden,
    down_sum,
    down_send,
    down_recv,
    load_sem,
    query_ssem,
    query_rsem,
    text_ssem,
    text_rsem,
    image_ssem,
    image_rsem,
    stat_ssem,
    stat_rsem,
    proj_ssem,
    proj_rsem,
    norm_ssem,
    norm_rsem,
    down_ssem,
    down_rsem,
):
    groups, depths, mps = dims
    pieces = groups * mps
    g = lax.axis_index("group")
    d = lax.axis_index("depth")
    m = lax.axis_index("mp")
    me = g * mps + m
    requests, heads, width = queries.shape
    kv_heads, span = text_keys.shape[1], text_keys.shape[2]
    share = heads // kv_heads
    stored, patches = image_keys.shape[0], image_keys.shape[2]
    listed = block_list.shape[1]
    steps = listed // depths
    copies = listed // (depths * groups)
    per_depth = requests // depths
    rows = states.shape[0]
    model = states.shape[1]
    scaling = 1.0 / math.sqrt(width)

    pairs = (
        (text_keys_hbm, text_keys),
        (text_values_hbm, text_values),
        (image_keys_hbm, image_keys),
        (image_values_hbm, image_values),
        (out_weight_hbm, out_weight),
        (gate_hbm, gate),
        (up_hbm, up),
        (down_hbm, down),
    )
    loads = [pltpu.make_async_copy(a, b, load_sem.at[i]) for i, (a, b) in enumerate(pairs)]
    for load in loads[:4]:
        load.start()

    barrier = pltpu.get_barrier_semaphore()

    def greet_piece(k, carry):
        peer = lax.rem(me + k, pieces)
        pl.semaphore_signal(
            barrier, inc=1, device_id=(peer // mps, d, lax.rem(peer, mps)), device_id_type=MESH
        )
        return carry

    lax.fori_loop(1, pieces, greet_piece, 0)
    for e in range(1, depths):

        def greet_depth(k, carry):
            pl.semaphore_signal(
                barrier,
                inc=1,
                device_id=(lax.rem(g + k, groups), lax.rem(d + e, depths), m),
                device_id_type=MESH,
            )
            return carry

        lax.fori_loop(0, groups, greet_depth, 0)

    own_count = block_count[g]

    def place_step(i, counts):
        out = []
        for p in range(depths):
            place = i * depths + p
            owner = image_slot[block_list[g, place]] // stored
            rank = jnp.int32(0)
            for o in range(groups):
                rank = jnp.where(owner == o, counts[p * groups + o], rank)
            codes[place] = jnp.minimum(owner * copies + rank, groups * copies - 1)
            live = (place < own_count).astype(jnp.int32)
            for o in range(groups):
                out.append(counts[p * groups + o] + jnp.where(owner == o, live, 0))
        return tuple(out)

    lax.fori_loop(0, steps, place_step, (jnp.int32(0),) * (depths * groups))

    def reader_step(r, found):
        for k in range(READS):
            place = image_first[r] + k
            held = jnp.minimum(place, listed - 1)
            good = (k < image_count[r]) & (place < own_count) & (lax.rem(place, depths) == d)
            code = jnp.where(good, codes[held], -1)
            found = tuple(jnp.where(code == i, r, old) for i, old in enumerate(found))
        return found

    found = lax.fori_loop(0, requests, reader_step, (jnp.int32(0),) * (groups * copies))
    for i, reader in enumerate(found):
        readers[i] = reader
    for o in range(groups):
        for c in range(copies):
            query_send[o, c] = queries[readers[o * copies + c]]
    query_recv[g] = query_send[g]

    pl.semaphore_wait(barrier, pieces - 1 + (depths - 1) * groups)

    def query_copy(peer, slot):
        return pltpu.make_async_remote_copy(
            src_ref=query_send.at[peer],
            dst_ref=query_recv.at[slot],
            send_sem=query_ssem.at[peer],
            recv_sem=query_rsem.at[slot],
            device_id=(peer, d, m),
            device_id_type=MESH,
        )

    def over(count, action):
        def body(k, carry):
            action(k)
            return carry

        lax.fori_loop(1, count, body, 0, unroll=True)

    over(groups, lambda k: query_copy(lax.rem(g + k, groups), g).start())

    def serve_step(i, state):
        place = i * depths + d
        out = []
        for s in range(groups):
            rank, picked = state[s]
            slot = image_slot[block_list[s, place]]
            hit = ((slot // stored) == g) & (place < block_count[s])
            within = lax.rem(slot, stored)
            target = jnp.where(hit, rank, -1)
            picked = tuple(jnp.where(target == c, within, old) for c, old in enumerate(picked))
            out.append((rank + hit.astype(jnp.int32), picked))
        return tuple(out)

    zero = jnp.int32(0)
    served = lax.fori_loop(0, steps, serve_step, ((zero, (zero,) * copies),) * groups)
    for s in range(groups):
        for c in range(copies):
            chosen[s * copies + c] = served[s][1][c]

    def by_head(parts):
        result = parts[0]
        row = lax.broadcasted_iota(jnp.int32, result.shape, 0)
        for h in range(1, kv_heads):
            result = jnp.where(row >= h * share, parts[h], result)
        return result

    def spread_rows(small):
        return by_head(
            [jnp.broadcast_to(small[h : h + 1, :], (heads, width)) for h in range(kv_heads)]
        )

    loads[0].wait()
    loads[4].start()
    lanes = lax.broadcasted_iota(jnp.int32, (heads, span), 1) + d * span

    def text_first(r, carry):
        q = queries[r]
        score = by_head(
            [
                lax.dot_general(q, text_keys[r, h], NT, preferred_element_type=F32)
                for h in range(kv_heads)
            ]
        )
        text_scores[r] = jnp.where(lanes < text_length[r], score * scaling, MASKED_SCORE)
        key = spread_rows(new_keys[r].astype(F32))
        new_score = jnp.sum(q.astype(F32) * key, axis=-1, keepdims=True) * scaling
        new_scores[r] = jnp.broadcast_to(new_score, (heads, width))
        return carry

    lax.fori_loop(0, requests, text_first, 0, unroll=4)
    is_first = jnp.full((requests, heads, width), d, jnp.int32) == 0
    score = text_scores[...]
    fresh = jnp.where(is_first, new_scores[...], MASKED_SCORE)
    top = jnp.maximum(jnp.max(score, axis=-1, keepdims=True), fresh)
    level = jnp.floor(top / LOG_TWO)
    text_part[:, 1] = level
    weight = jnp.where(
        score > 0.5 * MASKED_SCORE, jnp.exp(score - LOG_TWO * level[:, :, :1]), 0.0
    ).astype(BF16)
    text_weights[...] = weight
    fresh_weight = jnp.where(is_first, jnp.exp(new_scores[...] - LOG_TWO * level), 0.0)
    fresh_weight = fresh_weight.astype(BF16).astype(F32)
    new_scores[...] = fresh_weight
    text_part[:, 2] = jnp.sum(weight.astype(F32), axis=-1, keepdims=True) + fresh_weight
    loads[1].wait()

    def text_second(r, carry):
        w = text_weights[r]
        value = by_head(
            [
                jnp.dot(w, text_values[r, h], preferred_element_type=F32)
                for h in range(kv_heads)
            ]
        )
        text_part[r, 0] = value + new_scores[r] * spread_rows(new_values[r].astype(F32))
        return carry

    lax.fori_loop(0, requests, text_second, 0, unroll=4)

    def text_copy(peer, slot):
        return pltpu.make_async_remote_copy(
            src_ref=text_part.at[pl.ds(peer * per_depth, per_depth)],
            dst_ref=text_recv.at[slot],
            send_sem=text_ssem.at[peer],
            recv_sem=text_rsem.at[slot],
            device_id=(g, peer, m),
            device_id_type=MESH,
        )

    over(depths, lambda k: text_copy(lax.rem(d + k, depths), d).start())
    for load in loads[5:]:
        load.start()

    loads[2].wait()
    loads[3].wait()

    stat_lane = lax.broadcasted_iota(jnp.int32, (heads, width), 1)

    def serve(s):
        slots = [chosen[s * copies + c] for c in range(copies)]
        for c in range(copies):
            q = query_recv[s, c]
            image_scores[c] = scaling * by_head(
                [
                    lax.dot_general(q, image_keys[slots[c], h], NT, preferred_element_type=F32)
                    for h in range(kv_heads)
                ]
            )
        score = image_scores[...]
        level = jnp.floor(jnp.max(score, axis=-1, keepdims=True) / LOG_TWO)
        weight = jnp.exp(score - LOG_TWO * level).astype(BF16)
        image_weights[...] = weight
        total = jnp.sum(weight.astype(F32), axis=-1, keepdims=True)
        stats = jnp.zeros((heads, width), F32)
        for c in range(copies):
            stats = jnp.where(stat_lane == 2 * c, level[c], stats)
            stats = jnp.where(stat_lane == 2 * c + 1, total[c], stats)
        stat_send[s] = stats
        for c in range(copies):
            w = image_weights[c]
            image_send[s, c] = by_head(
                [
                    jnp.dot(w, image_values[slots[c], h], preferred_element_type=F32)
                    for h in range(kv_heads)
                ]
            ).astype(BF16)

    def image_copy(peer, depth, slot, slot_depth):
        return pltpu.make_async_remote_copy(
            src_ref=image_send.at[peer],
            dst_ref=image_recv.at[slot_depth, pl.ds(slot * copies, copies)],
            send_sem=image_ssem.at[depth, peer],
            recv_sem=image_rsem.at[slot_depth, slot],
            device_id=(peer, depth, m),
            device_id_type=MESH,
        )

    def stat_copy(peer, depth, slot, slot_depth):
        return pltpu.make_async_remote_copy(
            src_ref=stat_send.at[peer],
            dst_ref=stat_recv.at[slot_depth, slot],
            send_sem=stat_ssem.at[depth, peer],
            recv_sem=stat_rsem.at[slot_depth, slot],
            device_id=(peer, depth, m),
            device_id_type=MESH,
        )

    serve(g)
    stat_recv[d, g] = stat_send[g]
    image_recv[d, pl.ds(g * copies, copies)] = image_send[g]
    for e in range(1, depths):
        image_copy(g, lax.rem(d + e, depths), g, d).start()
        stat_copy(g, lax.rem(d + e, depths), g, d).start()

    def serve_other(k):
        s = lax.rem(g + k, groups)
        query_copy(s, s).wait_recv()
        serve(s)
        for e in range(depths):
            image_copy(s, lax.rem(d + e, depths), g, d).start()
            stat_copy(s, lax.rem(d + e, depths), g, d).start()

    over(groups, serve_other)

    over(depths, lambda k: text_copy(lax.rem(d + k, depths), lax.rem(d + k, depths)).wait_recv())
    for e in range(1, depths):
        other = lax.rem(d + e, depths)
        image_copy(g, other, g, other).wait_recv()
        stat_copy(g, other, g, other).wait_recv()

    def image_arrival(k):
        s = lax.rem(g + k, groups)
        for e in range(depths):
            other = lax.rem(d + e, depths)
            image_copy(s, other, s, other).wait_recv()
            stat_copy(s, other, s, other).wait_recv()

    over(groups, image_arrival)
    text_recv[d] = text_part[pl.ds(d * per_depth, per_depth)]

    def stat_of(stats, lane):
        picked = jnp.sum(jnp.where(stat_lane == lane, stats, 0.0), axis=-1, keepdims=True)
        return jnp.broadcast_to(picked, (heads, width))

    def merge(i, carry):
        r = d * per_depth + i
        parts = [tuple(text_recv[e, i, n] for n in range(3)) for e in range(depths)]
        for k in range(READS):
            place = image_first[r] + k
            good = (k < image_count[r]) & (place < own_count)
            held = jnp.minimum(place, listed - 1)
            code = codes[held]
            at = lax.rem(held, depths)
            stats = stat_recv[at, code // copies]
            rank = lax.rem(code, copies)
            live = jnp.full((heads, width), good.astype(jnp.int32), jnp.int32) == 1
            parts.append(
                (
                    jnp.where(live, image_recv[at, code].astype(F32), 0.0),
                    jnp.where(live, stat_of(stats, 2 * rank), MASKED_SCORE),
                    jnp.where(live, stat_of(stats, 2 * rank + 1), 0.0),
                )
            )
        highest = functools.reduce(jnp.maximum, [part[1] for part in parts])
        factors = [jnp.exp2(part[1] - highest) for part in parts]
        total = sum(part[2] * factor for part, factor in zip(parts, factors))
        value = sum(part[0] * factor for part, factor in zip(parts, factors)) / total
        merged[i] = value
        attention_out[i] = value.astype(BF16)
        return carry

    lax.fori_loop(0, per_depth, merge, 0, unroll=2)
    for h in range(heads):
        flat[:, h * width : (h + 1) * width] = merged[:, h, :]

    loads[4].wait()
    low = flat[...].astype(BF16)
    tile = tile_of(model, 512)

    def project(n, carry):
        columns = pl.ds(pl.multiple_of(n * tile, tile), tile)
        projected[:, columns] = jnp.dot(low, out_weight[:, columns], preferred_element_type=F32)
        return carry

    lax.fori_loop(0, model // tile, project, 0)
    for i in range(mps):
        proj_send[i] = projected[i * rows : (i + 1) * rows, :].astype(proj_send.dtype)

    def proj_copy(peer, slot):
        return pltpu.make_async_remote_copy(
            src_ref=proj_send.at[peer],
            dst_ref=proj_recv.at[slot],
            send_sem=proj_ssem.at[peer],
            recv_sem=proj_rsem.at[slot],
            device_id=(g, d, peer),
            device_id_type=MESH,
        )

    over(mps, lambda k: proj_copy(lax.rem(m + k, mps), m).start())
    proj_recv[m] = proj_send[m]
    over(mps, lambda k: proj_copy(lax.rem(m + k, mps), lax.rem(m + k, mps)).wait_recv())
    total = states[...].astype(F32)
    for i in range(mps):
        total = total + proj_recv[i].astype(F32)
    residual[...] = total
    spread = jnp.mean(total * total, axis=-1, keepdims=True)
    norm_all[me] = (total * lax.rsqrt(spread + NORM_EPSILON) * norm_gain[...]).astype(BF16)

    def norm_copy(peer, slot):
        return pltpu.make_async_remote_copy(
            src_ref=norm_all.at[me],
            dst_ref=norm_all.at[slot],
            send_sem=norm_ssem.at[peer],
            recv_sem=norm_rsem.at[slot],
            device_id=(peer // mps, d, lax.rem(peer, mps)),
            device_id_type=MESH,
        )

    over(pieces, lambda k: norm_copy(lax.rem(me + k, pieces), me).start())
    loads[5].wait()
    loads[6].wait()
    loads[7].wait()
    over(pieces, lambda k: norm_copy(lax.rem(me + k, pieces), lax.rem(me + k, pieces)).wait_recv())
    for i in range(pieces):
        tokens[i * rows : (i + 1) * rows, :] = norm_all[i].astype(F32)
    tokens_low[...] = tokens[...].astype(BF16)
    gate_sum[...] = jnp.zeros_like(gate_sum)
    up_sum[...] = jnp.zeros_like(up_sum)

    def expand(k, carry):
        part = pl.ds(pl.multiple_of(k * tile, tile), tile)
        x = tokens_low[:, part]
        gate_sum[...] += jnp.dot(x, gate[part, :], preferred_element_type=F32)
        up_sum[...] += jnp.dot(x, up[part, :], preferred_element_type=F32)
        return carry

    lax.fori_loop(0, model // tile, expand, 0)
    v = gate_sum[...]
    hidden[...] = (v / (1.0 + jnp.exp(-v)) * up_sum[...]).astype(BF16)

    def contract(n, carry):
        columns = pl.ds(pl.multiple_of(n * tile, tile), tile)
        down_sum[:, columns] = jnp.dot(hidden[...], down[:, columns], preferred_element_type=F32)
        return carry

    lax.fori_loop(0, model // tile, contract, 0)
    for i in range(pieces):
        down_send[i] = down_sum[i * rows : (i + 1) * rows, :].astype(down_send.dtype)

    def down_copy(peer, slot):
        return pltpu.make_async_remote_copy(
            src_ref=down_send.at[peer],
            dst_ref=down_recv.at[slot],
            send_sem=down_ssem.at[peer],
            recv_sem=down_rsem.at[slot],
            device_id=(peer // mps, d, lax.rem(peer, mps)),
            device_id_type=MESH,
        )

    over(pieces, lambda k: down_copy(lax.rem(me + k, pieces), me).start())
    down_recv[me] = down_send[me]
    over(pieces, lambda k: down_copy(lax.rem(me + k, pieces), lax.rem(me + k, pieces)).wait_recv())

    def add_piece(i, total):
        return total + down_recv[i].astype(F32)

    layer_out[...] = lax.fori_loop(0, pieces, add_piece, residual[...]).astype(BF16)

    over(groups, lambda k: query_copy(lax.rem(g + k, groups), g).wait_send())
    over(depths, lambda k: text_copy(lax.rem(d + k, depths), d).wait_send())
    for e in range(1, depths):
        image_copy(g, lax.rem(d + e, depths), g, d).wait_send()
        stat_copy(g, lax.rem(d + e, depths), g, d).wait_send()

    def image_gone(k):
        for e in range(depths):
            image_copy(lax.rem(g + k, groups), lax.rem(d + e, depths), g, d).wait_send()
            stat_copy(lax.rem(g + k, groups), lax.rem(d + e, depths), g, d).wait_send()

    over(groups, image_gone)
    over(mps, lambda k: proj_copy(lax.rem(m + k, mps), m).wait_send())
    over(pieces, lambda k: norm_copy(lax.rem(me + k, pieces), me).wait_send())
    over(pieces, lambda k: down_copy(lax.rem(me + k, pieces), me).wait_send())


def on_device(
    states,
    queries,
    new_keys,
    new_values,
    text_keys,
    text_values,
    text_length,
    image_keys,
    image_values,
    image_slot,
    block_list,
    block_count,
    image_first,
    image_count,
    out_weight,
    norm_gain,
    gate_weight,
    up_weight,
    down_weight,
):
    groups = lax.axis_size("group")
    depths = lax.axis_size("depth")
    mps = lax.axis_size("mp")
    pieces = groups * mps
    requests, heads, width = queries.shape
    listed = block_list.shape[1]
    copies = listed // (depths * groups)
    per_depth = requests // depths
    rows, model = states.shape
    units = gate_weight.shape[1]
    span = text_keys.shape[2]
    patches = image_keys.shape[2]
    dma = pltpu.SemaphoreType.DMA
    vmem = pl.BlockSpec(memory_space=pltpu.VMEM)
    smem = pl.BlockSpec(memory_space=pltpu.SMEM)
    hbm = pl.BlockSpec(memory_space=pl.ANY)
    big = (
        text_keys,
        text_values,
        image_keys,
        image_values,
        out_weight,
        gate_weight,
        up_weight,
        down_weight,
    )
    scratch = [pltpu.VMEM(a.shape, a.dtype) for a in big]
    scratch += [
        pltpu.SMEM((groups * copies,), jnp.int32),
        pltpu.SMEM((listed,), jnp.int32),
        pltpu.SMEM((groups * copies,), jnp.int32),
        pltpu.VMEM((groups, copies, heads, width), BF16),
        pltpu.VMEM((groups, copies, heads, width), BF16),
        pltpu.VMEM((requests, heads, span), F32),
        pltpu.VMEM((requests, heads, width), F32),
        pltpu.VMEM((requests, heads, span), BF16),
        pltpu.VMEM((requests, 3, heads, width), F32),
        pltpu.VMEM((depths, per_depth, 3, heads, width), F32),
        pltpu.VMEM((copies, heads, patches), F32),
        pltpu.VMEM((copies, heads, patches), BF16),
        pltpu.VMEM((groups, copies, heads, width), BF16),
        pltpu.VMEM((groups, heads, width), F32),
        pltpu.VMEM((depths, groups * copies, heads, width), BF16),
        pltpu.VMEM((depths, groups, heads, width), F32),
        pltpu.VMEM((per_depth, heads, width), F32),
        pltpu.VMEM((per_depth, heads * width), F32),
        pltpu.VMEM((per_depth, model), F32),
        pltpu.VMEM((mps, rows, model), BF16),
        pltpu.VMEM((mps, rows, model), BF16),
        pltpu.VMEM((rows, model), F32),
        pltpu.VMEM((pieces, rows, model), BF16),
        pltpu.VMEM((pieces * rows, model), F32),
        pltpu.VMEM((pieces * rows, model), BF16),
        pltpu.VMEM((pieces * rows, units), F32),
        pltpu.VMEM((pieces * rows, units), F32),
        pltpu.VMEM((pieces * rows, units), BF16),
        pltpu.VMEM((pieces * rows, model), F32),
        pltpu.VMEM((pieces, rows, model), BF16),
        pltpu.VMEM((pieces, rows, model), BF16),
        dma((len(big),)),
        dma((groups,)),
        dma((groups,)),
        dma((depths,)),
        dma((depths,)),
        dma((depths, groups)),
        dma((depths, groups)),
        dma((depths, groups)),
        dma((depths, groups)),
        dma((mps,)),
        dma((mps,)),
        dma((pieces,)),
        dma((pieces,)),
        dma((pieces,)),
        dma((pieces,)),
    ]
    return pl.pallas_call(
        functools.partial(kernel, (groups, depths, mps)),
        out_shape=(
            jax.ShapeDtypeStruct((per_depth, heads, width), BF16),
            jax.ShapeDtypeStruct((rows, model), BF16),
        ),
        in_specs=[vmem] * 5 + [smem] * 6 + [hbm] * 8,
        out_specs=(vmem, vmem),
        scratch_shapes=scratch,
        compiler_params=pltpu.CompilerParams(
            collective_id=0, has_side_effects=True, vmem_limit_bytes=67043328
        ),
    )(
        states,
        queries,
        new_keys,
        new_values,
        norm_gain.reshape(1, model),
        text_length,
        image_slot,
        block_list,
        block_count,
        image_first,
        image_count,
        *big,
    )


def solution(mesh):
    placed = (
        P(("group", "depth", "mp"), None),
        P("group", "mp", None),
        P("group", "mp", None),
        P("group", "mp", None),
        P("group", "mp", "depth", None),
        P("group", "mp", "depth", None),
        P("group"),
        P("group", "mp", None, None),
        P("group", "mp", None, None),
        P(),
        P(),
        P(),
        P("group"),
        P("group"),
        P("mp", None),
        P(),
        P(None, ("group", "mp")),
        P(None, ("group", "mp")),
        P(("group", "mp"), None),
    )
    return jax.shard_map(
        on_device,
        mesh=mesh,
        in_specs=placed,
        out_specs=(P(("group", "depth"), "mp", None), P(("group", "depth", "mp"), None)),
        check_vma=False,
    )
```
